32 devices in a mesh: dp: 32 (over z, y, x, core).
Axes of the slice: x: 2, y: 2, z: 4, core: 2. Of those that a mesh axis runs over, the one named last changes fastest.
Arguments:
- captions: bfloat16 [1024, 77, 768], P('dp'), may hold values from -6 to 6
- caption_layout: int32 [2, 1024], replicated, may hold values from 0 to 77, as said below
- images: bfloat16 [1024, 768], P('dp'), may hold values from -0.24 to 0.24
- w_query: bfloat16 [768, 768], replicated, may hold values from -0.21875 to 0.21875
- w_keyval: bfloat16 [768, 1536], replicated, may hold values from -0.21875 to 0.21875
- w_out: bfloat16 [768, 768], replicated, may hold values from -0.21875 to 0.21875
- w_up: bfloat16 [768, 3072], replicated, may hold values from -0.21875 to 0.21875
- w_down: bfloat16 [3072, 768], replicated, may hold values from -0.109375 to 0.109375
- w_proj: bfloat16 [768, 768], replicated, may hold values from -0.009114583 to 0.009114583
Outputs:
- image_grad: float32 [1024, 768], P('dp')
- text_grad: float32 [1024, 768], P('dp')
The draws below stay inside these ranges and needn't reach their ends.
Inputs may be any that keep to these rules, and one draw needn't show every extreme that they name: `caption_layout`: row 0 holds each caption's token count; row 1 is 1 where the caption is encoded by the next index of dp (index 0 after the last) and 0 where by its own. Exactly 8 of each device's captions carry 1. The captions one device encodes (its own that carry 0 and those carrying 1 of the index before it) hold at most 2048 tokens together, exactly that many on some device.
All inputs are finite; a program needn't handle non-finite values.
Results may differ from the reference program's by a relative error of at most 0.018.
Values may be sent and summed in bfloat16 or wider, within the bound.
A program may use at most 128 MiB of HBM per device.

```python
import math
import jax
import jax.numpy as jnp
from jax import lax

D = 768
HEADS = 12
FF = 3072
E = 768
CTX = 77
CAP_DEV = 32
HAND = 8
TOK_CAP = 2048
PAIRS = 1024
N_DP = 32


def caption_plan(key):
    order_key = jax.random.fold_in(key, 7102)
    length_key = jax.random.fold_in(key, 7103)
    heavy_key = jax.random.fold_in(key, 7104)
    hand_counts = jnp.full((N_DP,), HAND, jnp.int32)
    permuted = jax.vmap(lambda sub_key: jax.random.permutation(sub_key, CAP_DEV))(jax.random.split(order_key, N_DP))
    position_rank = jnp.argsort(permuted, axis=1)
    handed_flags = (position_rank < hand_counts[:, None]).astype(jnp.int32)
    owner_index = jnp.broadcast_to(jnp.arange(N_DP, dtype=jnp.int32)[:, None], (N_DP, CAP_DEV))
    group_index = ((owner_index + handed_flags) % N_DP).reshape(-1)
    heaviness = jax.random.randint(heavy_key, (N_DP, 1), 2, 5)
    raw_length = (jax.random.randint(length_key, (N_DP, CAP_DEV), 0, CTX) * heaviness // 4).reshape(-1)
    raw_length = jnp.where(group_index == 0, CTX - 1, raw_length)
    onehot = (group_index[:, None] == jnp.arange(N_DP, dtype=jnp.int32)[None, :]).astype(jnp.int32)
    members = jnp.sum(onehot, axis=0)
    total_raw = jnp.sum(onehot * raw_length[:, None], axis=0)
    room_left = TOK_CAP - members
    own_room = room_left[group_index]
    own_total = jnp.maximum(total_raw[group_index], 1)
    floor_part = raw_length * own_room // own_total
    floor_total = jnp.sum(onehot * floor_part[:, None], axis=0)
    group_rank = jnp.sum((jnp.cumsum(onehot, axis=0) - onehot) * onehot, axis=1)
    extra_token = (group_rank < (room_left - floor_total)[group_index]).astype(jnp.int32)
    scaled = (total_raw > room_left)[group_index]
    lengths = jnp.where(scaled, 1 + floor_part + extra_token, 1 + raw_length)
    return jnp.stack([lengths, handed_flags.reshape(-1)]).astype(jnp.int32)


def draw_caption_layout(key, part):
    return caption_plan(key)


def draw_captions(key, part):
    noise = jax.random.normal(jax.random.fold_in(key, 7211), (PAIRS, CTX, D), jnp.float32)
    values = jnp.clip(noise, -6.0, 6.0)
    return values.astype(jnp.bfloat16)


def draw_w_proj(key, part):
    noise = jax.random.normal(jax.random.fold_in(key, 7221), (D, E), jnp.float32)
    values = jnp.clip(noise, -6.0, 6.0) / math.sqrt(D * E)
    return values.astype(jnp.bfloat16)


def draw_images(key, part):
    noise = jax.random.normal(jax.random.fold_in(key, 7231), (PAIRS, E), jnp.float32)
    values = 0.04 * jnp.clip(noise, -5.9, 5.9)
    return values.astype(jnp.bfloat16)


def bell_draw(key, dims, scale, most, held_as=jnp.bfloat16):
    values = jax.random.normal(key, dims, jnp.float32) * scale
    return jnp.minimum(jnp.maximum(values, -most), most).astype(held_as)


def setup_inputs(seed: int = 0) -> dict:
    seeds = jax.random.split(jax.random.key(seed), 10)
    captions = draw_captions(jax.random.fold_in(seeds[9], 71), 0)
    caption_layout = draw_caption_layout(jax.random.fold_in(seeds[9], 71), 0)
    images = draw_images(jax.random.fold_in(seeds[9], 71), 0)
    w_query = bell_draw(seeds[3], (D, D), D ** -0.5, 0.21875)
    w_keyval = bell_draw(seeds[4], (D, 2 * D), D ** -0.5, 0.21875)
    w_out = bell_draw(seeds[5], (D, D), D ** -0.5, 0.21875)
    w_up = bell_draw(seeds[6], (D, FF), D ** -0.5, 0.21875)
    w_down = bell_draw(seeds[7], (FF, D), FF ** -0.5, 0.109375)
    w_proj = draw_w_proj(jax.random.fold_in(seeds[9], 71), 0)
    return dict(captions=captions, caption_layout=caption_layout, images=images, w_query=w_query, w_keyval=w_keyval, w_out=w_out, w_up=w_up, w_down=w_down, w_proj=w_proj)


LOGIT_SCALE = 100.0
EPS_NORM = 1e-05
EPS_UNIT = 1e-06

def layer_norm(values):
    values = values.astype(jnp.float32)
    center = values - lax.optimization_barrier(jnp.mean(values, axis=-1, keepdims=True))
    spread = lax.optimization_barrier(jnp.mean(center * center, axis=-1, keepdims=True))
    return center * lax.rsqrt(spread + EPS_NORM)

def unit_rows(values):
    values = values.astype(jnp.float32)
    return values * lax.rsqrt(lax.optimization_barrier(jnp.sum(values * values, axis=-1, keepdims=True)) + EPS_UNIT)

def contract_first(left, right):
    return lax.dot_general(left, right, (((0,), (0,)), ((), ())), preferred_element_type=jnp.float32)

def contract_last(left, right):
    return lax.dot_general(left, right, (((1,), (1,)), ((), ())), preferred_element_type=jnp.float32)

def reference(captions, caption_layout, images, w_query, w_keyval, w_out, w_up, w_down, w_proj):
    model_width = captions.shape[2]
    head_dim = model_width // HEADS

    def encode_block(block_item):
        caption_block, block_lengths = block_item
        block_count = caption_block.shape[0]
        normed = layer_norm(caption_block).astype(jnp.bfloat16)
        keyval = jnp.dot(normed.reshape(-1, model_width), w_keyval, preferred_element_type=jnp.float32)
        keyval = keyval.astype(jnp.bfloat16).reshape(block_count, CTX, 2 * model_width)
        last_slot = (block_lengths - 1).astype(jnp.int32)[:, None, None]
        end_normed = jnp.take_along_axis(normed, last_slot, axis=1)[:, 0]
        end_tokens = jnp.take_along_axis(caption_block, last_slot, axis=1)[:, 0]
        query = jnp.dot(end_normed, w_query, preferred_element_type=jnp.float32).astype(jnp.bfloat16)
        key_heads = keyval[:, :, :model_width].reshape(block_count, CTX, HEADS, head_dim).astype(jnp.float32)
        value_heads = keyval[:, :, model_width:].reshape(block_count, CTX, HEADS, head_dim).astype(jnp.float32)
        query_heads = query.reshape(block_count, HEADS, head_dim).astype(jnp.float32)
        scores = jnp.einsum('chd,cthd->cht', query_heads, key_heads) / math.sqrt(head_dim)
        inside = jnp.arange(CTX)[None, None, :] < block_lengths[:, None, None]
        masked = jnp.where(inside, scores, -jnp.inf)
        peak = lax.optimization_barrier(jnp.max(masked, axis=-1, keepdims=True))
        exponent = jnp.exp(masked - peak)
        attention = (exponent / lax.optimization_barrier(jnp.sum(exponent, axis=-1, keepdims=True))).astype(jnp.bfloat16)
        mixed_heads = jnp.einsum('cht,cthd->chd', attention.astype(jnp.float32), value_heads)
        mixed_heads = mixed_heads.astype(jnp.bfloat16).reshape(block_count, model_width)
        residual = end_tokens.astype(jnp.float32) + jnp.dot(mixed_heads, w_out, preferred_element_type=jnp.float32)
        residual = residual.astype(jnp.bfloat16)
        inner_norm = layer_norm(residual).astype(jnp.bfloat16)
        hidden = jax.nn.gelu(jnp.dot(inner_norm, w_up, preferred_element_type=jnp.float32), approximate=False)
        hidden = hidden.astype(jnp.bfloat16)
        final_rows = residual.astype(jnp.float32) + jnp.dot(hidden, w_down, preferred_element_type=jnp.float32)
        pooled = layer_norm(final_rows).astype(jnp.bfloat16)
        return jnp.dot(pooled, w_proj, preferred_element_type=jnp.float32).astype(jnp.bfloat16)
    caption_blocks = captions.reshape(N_DP, CAP_DEV, CTX, model_width)
    length_blocks = caption_layout[0].reshape(N_DP, CAP_DEV)
    text_embed = lax.map(encode_block, (caption_blocks, length_blocks)).reshape(PAIRS, -1)
    image_unit = unit_rows(images).astype(jnp.bfloat16)
    text_unit = unit_rows(text_embed).astype(jnp.bfloat16)
    scores = LOGIT_SCALE * contract_last(image_unit, text_unit)
    row_peak = lax.optimization_barrier(jnp.max(scores, axis=1, keepdims=True))
    row_logsum = row_peak[:, 0] + jnp.log(lax.optimization_barrier(jnp.sum(jnp.exp(scores - row_peak), axis=1)))
    column_peak = lax.optimization_barrier(jnp.max(scores, axis=0, keepdims=True))
    column_logsum = column_peak[0] + jnp.log(lax.optimization_barrier(jnp.sum(jnp.exp(scores - column_peak), axis=0)))
    row_weights = jnp.exp(scores - row_logsum[:, None]).astype(jnp.bfloat16)
    column_weights = jnp.exp(scores - column_logsum[None, :]).astype(jnp.bfloat16)
    half_scale = 0.5 * LOGIT_SCALE
    image_unit_grad = half_scale * (jnp.dot(row_weights, text_unit, preferred_element_type=jnp.float32) + jnp.dot(column_weights, text_unit, preferred_element_type=jnp.float32))
    image_unit_grad = image_unit_grad - LOGIT_SCALE * text_unit.astype(jnp.float32)
    text_unit_grad = half_scale * (contract_first(row_weights, image_unit) + contract_first(column_weights, image_unit))
    text_unit_grad = text_unit_grad - LOGIT_SCALE * image_unit.astype(jnp.float32)
    image_value, image_back = jax.vjp(unit_rows, images.astype(jnp.float32))
    text_value, text_back = jax.vjp(unit_rows, text_embed.astype(jnp.float32))
    return (image_back(image_unit_grad)[0], text_back(text_unit_grad)[0])
```

```python
import functools

import jax
import jax.numpy as jnp
from jax import lax
from jax.experimental import pallas as pl
from jax.experimental.pallas import tpu as pltpu
from jax.sharding import PartitionSpec as P

HEADS = 12
LOGIT_SCALE = 100.0
EPS_NORM = 1e-05
EPS_UNIT = 1e-06
GROUP = 8
QUAD = 4
LSE_BLOCK = 256
FF_CHUNKS = 4
MESH = pl.DeviceIdType.MESH
F32 = jnp.float32
BF16 = jnp.bfloat16


def dot(a, b):
    return jnp.dot(a, b, preferred_element_type=F32)


def dot_last(a, b):
    return lax.dot_general(a, b, (((1,), (1,)), ((), ())), preferred_element_type=F32)


def dot_first(a, b):
    return lax.dot_general(a, b, (((0,), (0,)), ((), ())), preferred_element_type=F32)


def layer_norm(x):
    center = x - jnp.mean(x, axis=-1, keepdims=True)
    spread = jnp.mean(center * center, axis=-1, keepdims=True)
    return center * lax.rsqrt(spread + EPS_NORM)


def unit_rows(x):
    return x * lax.rsqrt(jnp.sum(x * x, axis=-1, keepdims=True) + EPS_UNIT)


def unit_back(x, g):
    s = jnp.sum(x * x, axis=-1, keepdims=True) + EPS_UNIT
    r = lax.rsqrt(s)
    return g * r - x * (jnp.sum(x * g, axis=-1, keepdims=True) * (r / s))


def kernel(
    n,
    cap_hbm, layout, images, wq_hbm, wkv_hbm, wo_hbm, wup_hbm, wdown_hbm, wproj_hbm,
    image_out, text_out,
    cap, normed, x_last, qk, mix, wq, wkv, wo, wup, wdown, wproj,
    gi, gt, row_lse, col_lse,
    load_sem, i_send, i_recv, i_rsend, i_rrecv, t_send, t_recv, t_rsend, t_rrecv,
):
    me = lax.axis_index("dp")
    half = n // 2
    partner = me + 1 - 2 * lax.rem(me, 2)
    caps, ctx, width = cap.shape
    groups = caps // GROUP
    slot = normed.shape[0] // caps
    head_dim = width // HEADS
    ff = wup.shape[1]
    fc = ff // FF_CHUNKS

    loads = []

    def load(src, dst):
        copy = pltpu.make_async_copy(src, dst, load_sem.at[len(loads)])
        copy.start()
        loads.append(copy)
        return copy

    cap_loads = [
        load(cap_hbm.at[pl.ds(g * GROUP, GROUP)], cap.at[pl.ds(g * GROUP, GROUP)])
        for g in range(groups)
    ]
    wq_load = load(wq_hbm, wq)
    wkv_load = load(wkv_hbm, wkv)
    wo_load = load(wo_hbm, wo)
    ff_loads = []
    for f in range(FF_CHUNKS):
        cols = pl.ds(f * fc, fc)
        ff_loads.append(
            (load(wup_hbm.at[:, cols], wup.at[:, cols]), load(wdown_hbm.at[cols], wdown.at[cols]))
        )
    wproj_load = load(wproj_hbm, wproj)

    barrier = pltpu.get_barrier_semaphore()

    def greet(k, carry):
        pl.semaphore_signal(
            barrier, inc=1, device_id=(lax.rem(me + 2 * k, n),), device_id_type=MESH
        )
        return carry

    lax.fori_loop(1, half, greet, 0)
    pl.semaphore_signal(barrier, inc=1, device_id=(partner,), device_id_type=MESH)

    def remote(buf, block, send, recv, target):
        return pltpu.make_async_remote_copy(
            src_ref=buf.at[block], dst_ref=buf.at[block], send_sem=send, recv_sem=recv,
            device_id=(target,), device_id_type=MESH,
        )

    def push(buf, send, recv, rsend, rrecv):
        def step(k, carry):
            remote(buf, me, send.at[k], recv.at[k], lax.rem(me + 2 * k, n)).start()
            return carry

        lax.fori_loop(1, half, step, 0)
        remote(buf, me, rsend.at[0], rrecv.at[0], partner).start()

    def relay(buf, send, recv, rsend, rrecv):
        def step(k, carry):
            block = lax.rem(me + n - 2 * k, n)
            remote(buf, block, send.at[k], recv.at[k], partner).wait_recv()
            remote(buf, block, rsend.at[k], rrecv.at[k], partner).start()
            return carry

        lax.fori_loop(1, half, step, 0)

    def finish(buf, send, recv, rsend, rrecv):
        def step(k, carry):
            block = lax.rem(partner + n - 2 * k, n)
            remote(buf, block, rsend.at[k], rrecv.at[k], partner).wait_recv()
            return carry

        lax.fori_loop(0, half, step, 0)

    def drain(buf, send, recv, rsend, rrecv):
        def step(k, carry):
            block = lax.rem(me + n - 2 * k, n)
            remote(buf, me, send.at[k], recv.at[k], partner).wait_send()
            remote(buf, block, rsend.at[k], rrecv.at[k], partner).wait_send()
            return carry

        lax.fori_loop(1, half, step, 0)
        remote(buf, me, rsend.at[0], rrecv.at[0], partner).wait_send()

    i_set = (gi, i_send, i_recv, i_rsend, i_rrecv)
    t_set = (gt, t_send, t_recv, t_rsend, t_rrecv)

    image = images[...].astype(F32)
    image_unit = unit_rows(image).astype(BF16)
    gi[me] = image_unit
    pl.semaphore_wait(barrier, half)
    push(*i_set)

    token = lax.broadcasted_iota(jnp.int32, (ctx, width), 0)
    tail = (ctx // 16) * 16
    for g in range(groups):
        cap_loads[g].wait()

        def norm_one(i, carry, g=g):
            c = g * GROUP + i
            x = cap[c].astype(F32)
            length = layout[0, me * caps + c]
            x_last[pl.ds(c, 1), :] = jnp.sum(
                jnp.where(token == length - 1, x, 0.0), axis=0, keepdims=True
            )
            base = pl.multiple_of(c * slot, 16)
            y = layer_norm(x).astype(BF16)
            normed[pl.ds(base, tail), :] = y[:tail]
            rest = jnp.concatenate(
                [y[tail:].astype(F32), jnp.zeros((slot - ctx, width), F32)], axis=0
            )
            normed[pl.ds(pl.multiple_of(base + tail, 16), slot - tail), :] = rest.astype(BF16)
            return carry

        lax.fori_loop(0, GROUP, norm_one, 0)

    last = x_last[...]
    last_normed = layer_norm(last).astype(BF16)
    wq_load.wait()
    query = dot(last_normed, wq[...]).astype(BF16).astype(F32) * (head_dim ** -0.5)
    wkv_load.wait()
    span = QUAD * head_dim
    lane = lax.broadcasted_iota(jnp.int32, (caps, span), 1)
    for b in range(HEADS // QUAD):
        piece = query[:, b * span : (b + 1) * span]
        stacked = jnp.concatenate(
            [
                jnp.where((lane >= j * head_dim) & (lane < (j + 1) * head_dim), piece, 0.0)
                for j in range(QUAD)
            ],
            axis=0,
        ).astype(BF16)
        part = dot_last(stacked, wkv[:, b * span : (b + 1) * span])
        qk[b * QUAD : (b + 1) * QUAD] = part.reshape(QUAD, caps, width)

    cols = HEADS * GROUP
    col_cap = lax.rem(lax.broadcasted_iota(jnp.int32, (1, cols), 1), GROUP)

    def attend(g, carry):
        base = pl.multiple_of(g * (GROUP * slot), 16)
        rows = normed[pl.ds(base, GROUP * slot), :]
        first = pl.multiple_of(g * GROUP, GROUP)
        keys = qk[:, pl.ds(first, GROUP), :].reshape(cols, width).astype(BF16)
        scores = dot_last(rows, keys)
        lengths = jnp.zeros((1, cols), jnp.int32)
        for i in range(GROUP):
            lengths = jnp.where(col_cap == i, layout[0, me * caps + g * GROUP + i], lengths)
        place = lax.broadcasted_iota(jnp.int32, scores.shape, 0) - col_cap * slot
        inside = (place >= 0) & (place < lengths)
        scores = jnp.where(inside, scores, -1e30)
        peak = jnp.max(scores, axis=0, keepdims=True)
        expo = jnp.where(inside, jnp.exp(scores - peak), 0.0)
        attn = (expo / jnp.sum(expo, axis=0, keepdims=True)).astype(BF16)
        mix[:, pl.ds(first, GROUP), :] = dot_first(attn, rows).reshape(HEADS, GROUP, width)
        return carry

    lax.fori_loop(0, groups, attend, 0)

    pieces = []
    for b in range(HEADS // QUAD):
        left = mix[b * QUAD : (b + 1) * QUAD].reshape(QUAD * caps, width).astype(BF16)
        wide = dot(left, wkv[:, width + b * span : width + (b + 1) * span])
        piece = wide[:caps]
        for j in range(1, QUAD):
            piece = jnp.where(lane >= j * head_dim, wide[j * caps : (j + 1) * caps], piece)
        pieces.append(piece)
    mixed = jnp.concatenate(pieces, axis=1).astype(BF16)
    wo_load.wait()
    residual = (last + dot(mixed, wo[...])).astype(BF16).astype(F32)
    inner = layer_norm(residual).astype(BF16)

    relay(*i_set)

    final = residual
    for f in range(FF_CHUNKS):
        up_load, down_load = ff_loads[f]
        up_load.wait()
        up = dot(inner, wup[:, f * fc : (f + 1) * fc])
        hidden = (0.5 * up * (1.0 + lax.erf(up * (2.0 ** -0.5)))).astype(BF16)
        down_load.wait()
        final = final + dot(hidden, wdown[f * fc : (f + 1) * fc])
    pooled = layer_norm(final).astype(BF16)
    wproj_load.wait()
    text = dot(pooled, wproj[...]).astype(BF16).astype(F32)
    text_unit = unit_rows(text).astype(BF16)
    gt[me] = text_unit
    push(*t_set)
    finish(*i_set)
    relay(*t_set)
    finish(*t_set)

    pairs = gi.shape[0] * gi.shape[1]
    step_blocks = LSE_BLOCK // caps

    def lse_block(b, carry):
        where = pl.ds(pl.multiple_of(b * LSE_BLOCK, LSE_BLOCK), LSE_BLOCK)
        for big, small, out in ((gi, gt, col_lse), (gt, gi, row_lse)):
            all_rows = big[...].reshape(pairs, width)
            block = small[pl.ds(b * step_blocks, step_blocks)].reshape(LSE_BLOCK, width)
            s = LOGIT_SCALE * dot_last(all_rows, block)
            peak = jnp.max(s, axis=0, keepdims=True)
            out[:, where] = peak + jnp.log(jnp.sum(jnp.exp(s - peak), axis=0, keepdims=True))
        return carry

    lax.fori_loop(0, pairs // LSE_BLOCK, lse_block, 0)

    half_scale = 0.5 * LOGIT_SCALE

    def grads(mine, others, other_lse, opposite):
        every = others[...].reshape(pairs, width)
        s = LOGIT_SCALE * dot_last(mine, every)
        peak = jnp.max(s, axis=1, keepdims=True)
        own = peak + jnp.log(jnp.sum(jnp.exp(s - peak), axis=1, keepdims=True))
        weights = jnp.concatenate(
            [jnp.exp(s - own), jnp.exp(s - other_lse)], axis=0
        ).astype(BF16)
        both = dot(weights, every)
        total = both[:caps] + both[caps:]
        return half_scale * total - LOGIT_SCALE * opposite.astype(F32)

    image_out[...] = unit_back(image, grads(image_unit, gt, col_lse[...], text_unit))
    text_out[...] = unit_back(text, grads(text_unit, gi, row_lse[...], image_unit))
    drain(*i_set)
    drain(*t_set)


def body(captions, caption_layout, images, w_query, w_keyval, w_out, w_up, w_down, w_proj):
    caps, ctx, width = captions.shape
    n = lax.axis_size("dp")
    slot = -(-ctx // 16) * 16
    half = n // 2
    pairs = n * caps
    loads = caps // GROUP + 4 + 2 * FF_CHUNKS
    any_spec = pl.BlockSpec(memory_space=pl.ANY)
    vmem = pl.BlockSpec(memory_space=pltpu.VMEM)
    smem = pl.BlockSpec(memory_space=pltpu.SMEM)
    out = jax.ShapeDtypeStruct(images.shape, F32)
    dma = pltpu.SemaphoreType.DMA
    return pl.pallas_call(
        functools.partial(kernel, n),
        out_shape=(out, out),
        in_specs=[any_spec, smem, vmem] + [any_spec] * 6,
        out_specs=(vmem, vmem),
        scratch_shapes=[
            pltpu.VMEM(captions.shape, BF16),
            pltpu.VMEM((caps * slot, width), BF16),
            pltpu.VMEM((caps, width), F32),
            pltpu.VMEM((HEADS, caps, width), F32),
            pltpu.VMEM((HEADS, caps, width), F32),
            pltpu.VMEM(w_query.shape, BF16),
            pltpu.VMEM(w_keyval.shape, BF16),
            pltpu.VMEM(w_out.shape, BF16),
            pltpu.VMEM(w_up.shape, BF16),
            pltpu.VMEM(w_down.shape, BF16),
            pltpu.VMEM(w_proj.shape, BF16),
            pltpu.VMEM((n, caps, width), BF16),
            pltpu.VMEM((n, caps, width), BF16),
            pltpu.VMEM((1, pairs), F32),
            pltpu.VMEM((1, pairs), F32),
            dma((loads,)),
        ]
        + [dma((half,)) for _ in range(8)],
        compiler_params=pltpu.CompilerParams(
            collective_id=0, has_side_effects=True, vmem_limit_bytes=64000000
        ),
    )(captions, caption_layout, images, w_query, w_keyval, w_out, w_up, w_down, w_proj)


def solution(mesh):
    return jax.shard_map(
        body,
        mesh=mesh,
        in_specs=(P("dp", None, None), P(), P("dp", None), P(), P(), P(), P(), P(), P()),
        out_specs=(P("dp", None), P("dp", None)),
        check_vma=False,
    )
```

```python
import functools

import jax
import jax.numpy as jnp
from jax import lax
from jax.experimental import pallas as pl
from jax.experimental.pallas import tpu as pltpu
from jax.sharding import PartitionSpec as P

HEADS = 12
LOGIT_SCALE = 100.0
EPS_NORM = 1e-05
EPS_UNIT = 1e-06
GROUP = 16
CAP_CHUNKS = 11
QUAD = 4
FF_CHUNKS = 4
MESH = pl.DeviceIdType.MESH
F32 = jnp.float32
BF16 = jnp.bfloat16


def dot(a, b):
    return jnp.dot(a, b, preferred_element_type=F32)


def dot_last(a, b):
    return lax.dot_general(a, b, (((1,), (1,)), ((), ())), preferred_element_type=F32)


def dot_first(a, b):
    return lax.dot_general(a, b, (((0,), (0,)), ((), ())), preferred_element_type=F32)


def layer_norm(x):
    center = x - jnp.mean(x, axis=-1, keepdims=True)
    spread = jnp.mean(center * center, axis=-1, keepdims=True)
    return center * lax.rsqrt(spread + EPS_NORM)


def unit_rows(x):
    return x * lax.rsqrt(jnp.sum(x * x, axis=-1, keepdims=True) + EPS_UNIT)


def unit_back(x, g):
    s = jnp.sum(x * x, axis=-1, keepdims=True) + EPS_UNIT
    r = lax.rsqrt(s)
    return g * r - x * (jnp.sum(x * g, axis=-1, keepdims=True) * (r / s))


def kernel(
    n,
    cap_hbm, layout, images, wq_hbm, wkv_hbm, wo_hbm, wup_hbm, wdown_hbm, wproj_hbm,
    image_out, text_out,
    cap, normed, qk, mix, wq, wkv, wo, wup, wdown, wproj,
    gi, gt, lse,
    load_sem, l_send, l_recv, i_send, i_recv, i_rsend, i_rrecv, t_send, t_recv, t_rsend, t_rrecv,
):
    me = lax.axis_index("dp")
    half = n // 2
    partner = me + 1 - 2 * lax.rem(me, 2)
    ctx, caps, width = cap.shape
    groups = caps // GROUP
    head_dim = width // HEADS
    ff = wup.shape[1]
    fc = ff // FF_CHUNKS

    loads = []

    def load(src, dst):
        copy = pltpu.make_async_copy(src, dst, load_sem.at[len(loads)])
        copy.start()
        loads.append(copy)
        return copy

    cap_steps = ctx // CAP_CHUNKS
    cap_loads = [
        load(cap_hbm.at[pl.ds(i * cap_steps, cap_steps)], cap.at[pl.ds(i * cap_steps, cap_steps)])
        for i in range(CAP_CHUNKS)
    ]
    wq_load = load(wq_hbm, wq)
    wkv_load = load(wkv_hbm, wkv)
    wo_load = load(wo_hbm, wo)
    ff_loads = []
    for f in range(FF_CHUNKS):
        cols = pl.ds(f * fc, fc)
        ff_loads.append(
            (load(wup_hbm.at[:, cols], wup.at[:, cols]), load(wdown_hbm.at[cols], wdown.at[cols]))
        )
    wproj_load = load(wproj_hbm, wproj)

    barrier = pltpu.get_barrier_semaphore()

    def greet(k, carry):
        pl.semaphore_signal(
            barrier, inc=1, device_id=(lax.rem(me + k, n),), device_id_type=MESH
        )
        return carry

    lax.fori_loop(1, n, greet, 0)

    def remote(buf, block, send, recv, target):
        return pltpu.make_async_remote_copy(
            src_ref=buf.at[block], dst_ref=buf.at[block], send_sem=send, recv_sem=recv,
            device_id=(target,), device_id_type=MESH,
        )

    def push(buf, send, recv, rsend, rrecv):
        def step(k, carry):
            remote(buf, me, send.at[k], recv.at[k], lax.rem(me + 2 * k, n)).start()
            return carry

        lax.fori_loop(1, half, step, 0)
        remote(buf, me, rsend.at[0], rrecv.at[0], partner).start()

    def relay(buf, send, recv, rsend, rrecv):
        def step(k, carry):
            block = lax.rem(me + n - 2 * k, n)
            remote(buf, block, send.at[k], recv.at[k], partner).wait_recv()
            remote(buf, block, rsend.at[k], rrecv.at[k], partner).start()
            return carry

        lax.fori_loop(1, half, step, 0)

    def finish(buf, send, recv, rsend, rrecv):
        def step(k, carry):
            block = lax.rem(partner + n - 2 * k, n)
            remote(buf, block, rsend.at[k], rrecv.at[k], partner).wait_recv()
            return carry

        lax.fori_loop(0, half, step, 0)

    def drain(buf, send, recv, rsend, rrecv):
        def step(k, carry):
            block = lax.rem(me + n - 2 * k, n)
            remote(buf, me, send.at[k], recv.at[k], partner).wait_send()
            remote(buf, block, rsend.at[k], rrecv.at[k], partner).wait_send()
            return carry

        lax.fori_loop(1, half, step, 0)
        remote(buf, me, rsend.at[0], rrecv.at[0], partner).wait_send()

    i_set = (gi, i_send, i_recv, i_rsend, i_rrecv)
    t_set = (gt, t_send, t_recv, t_rsend, t_rrecv)

    image = images[...].astype(F32)
    image_unit = unit_rows(image).astype(BF16)
    gi[me] = image_unit
    pl.semaphore_wait(barrier, n - 1)
    push(*i_set)

    row = lax.broadcasted_iota(jnp.int32, (caps, 128), 0)
    length_rows = jnp.zeros((caps, 128), jnp.int32)
    for c in range(caps):
        length_rows = jnp.where(row == c, layout[0, me * caps + c], length_rows)
    length_rows = jnp.concatenate([length_rows] * (width // 128), axis=1)

    last = jnp.zeros((caps, width), F32)
    for i in range(CAP_CHUNKS):
        cap_loads[i].wait()
        for t in range(i * cap_steps, (i + 1) * cap_steps):
            x = cap[t].astype(F32)
            last = jnp.where(length_rows == t + 1, x, last)
            y = layer_norm(x).astype(BF16)
            for g in range(groups):
                normed[g, t] = y[g * GROUP : (g + 1) * GROUP]
    last_normed = layer_norm(last).astype(BF16)
    wq_load.wait()
    query = dot(last_normed, wq[...]).astype(BF16).astype(F32) * (head_dim ** -0.5)
    wkv_load.wait()
    span = QUAD * head_dim
    lane = lax.broadcasted_iota(jnp.int32, (caps, span), 1)
    for b in range(HEADS // QUAD):
        piece = query[:, b * span : (b + 1) * span]
        stacked = jnp.concatenate(
            [
                jnp.where((lane >= j * head_dim) & (lane < (j + 1) * head_dim), piece, 0.0)
                for j in range(QUAD)
            ],
            axis=0,
        ).astype(BF16)
        part = dot_last(stacked, wkv[:, b * span : (b + 1) * span])
        qk[b * QUAD : (b + 1) * QUAD] = part.reshape(QUAD, caps, width)

    cols = HEADS * GROUP
    col_cap = lax.rem(lax.broadcasted_iota(jnp.int32, (1, cols), 1), GROUP)
    row_index = lax.broadcasted_iota(jnp.int32, (ctx * GROUP, cols), 0)
    same = lax.rem(row_index, GROUP) == col_cap

    for g in range(groups):
        rows = normed[g].reshape(ctx * GROUP, width)
        keys = qk[:, g * GROUP : (g + 1) * GROUP, :].reshape(cols, width).astype(BF16)
        scores = dot_last(rows, keys)
        lengths = jnp.zeros((1, cols), jnp.int32)
        for i in range(GROUP):
            lengths = jnp.where(col_cap == i, layout[0, me * caps + g * GROUP + i], lengths)
        inside = same & (row_index < lengths * GROUP)
        scores = jnp.where(inside, scores, -1e30)
        peak = jnp.max(scores, axis=0, keepdims=True)
        expo = jnp.where(inside, jnp.exp(scores - peak), 0.0)
        attn = (expo / jnp.sum(expo, axis=0, keepdims=True)).astype(BF16)
        mix[:, g * GROUP : (g + 1) * GROUP, :] = dot_first(attn, rows).reshape(HEADS, GROUP, width)

    pieces = []
    for b in range(HEADS // QUAD):
        left = mix[b * QUAD : (b + 1) * QUAD].reshape(QUAD * caps, width).astype(BF16)
        wide = dot(left, wkv[:, width + b * span : width + (b + 1) * span])
        piece = wide[:caps]
        for j in range(1, QUAD):
            piece = jnp.where(lane >= j * head_dim, wide[j * caps : (j + 1) * caps], piece)
        pieces.append(piece)
    mixed = jnp.concatenate(pieces, axis=1).astype(BF16)
    wo_load.wait()
    residual = (last + dot(mixed, wo[...])).astype(BF16).astype(F32)
    inner = layer_norm(residual).astype(BF16)

    relay(*i_set)

    final = residual
    for f in range(FF_CHUNKS):
        up_load, down_load = ff_loads[f]
        up_load.wait()
        up = dot(inner, wup[:, f * fc : (f + 1) * fc])
        hidden = (0.5 * up * (1.0 + lax.erf(up * (2.0 ** -0.5)))).astype(BF16)
        down_load.wait()
        final = final + dot(hidden, wdown[f * fc : (f + 1) * fc])
    pooled = layer_norm(final).astype(BF16)
    wproj_load.wait()
    text = dot(pooled, wproj[...]).astype(BF16).astype(F32)
    text_unit = unit_rows(text).astype(BF16)
    gt[me] = text_unit
    push(*t_set)
    finish(*i_set)

    pairs = gi.shape[0] * gi.shape[1]
    per_row = 128 // caps
    spot = lax.broadcasted_iota(jnp.int32, (caps, 128), 1) - lax.rem(me, per_row) * caps
    here = spot == row

    def score(mine, others):
        s = LOGIT_SCALE * dot_last(mine, others[...].reshape(pairs, width))
        peak = jnp.max(s, axis=1, keepdims=True)
        own = peak + jnp.log(jnp.sum(jnp.exp(s - peak), axis=1, keepdims=True))
        return s, own

    def pull(s, logsum, others):
        weights = jnp.exp(s - logsum).astype(BF16)
        return dot(weights, others[...].reshape(pairs, width))

    def as_lanes(own):
        return jnp.sum(jnp.where(here, own, 0.0), axis=0, keepdims=True)

    text_scores, col_own = score(text_unit, gi)
    text_pull = pull(text_scores, col_own, gi)
    relay(*t_set)
    finish(*t_set)
    image_scores, row_own = score(image_unit, gt)
    lse[me] = jnp.concatenate([as_lanes(row_own), as_lanes(col_own)], axis=0)

    def lse_copy(k, block, target):
        return pltpu.make_async_remote_copy(
            src_ref=lse.at[block], dst_ref=lse.at[block], send_sem=l_send.at[k],
            recv_sem=l_recv.at[k], device_id=(target,), device_id_type=MESH,
        )

    def lse_send(k, carry):
        lse_copy(k, me, lax.rem(me + k, n)).start()
        return carry

    def lse_wait(k, carry):
        lse_copy(k, lax.rem(me + n - k, n), partner).wait_recv()
        return carry

    def lse_drain(k, carry):
        lse_copy(k, me, partner).wait_send()
        return carry

    lax.fori_loop(1, n, lse_send, 0)
    image_pull = pull(image_scores, row_own, gt)
    lax.fori_loop(1, n, lse_wait, 0)
    rows_cols = [
        sum(lse[d] for d in range(start, start + per_row)) for start in range(0, n, per_row)
    ]
    every = jnp.concatenate(rows_cols, axis=1)
    image_pull = image_pull + pull(image_scores, every[1:2], gt)
    text_pull = text_pull + pull(text_scores, every[0:1], gi)

    def finish_grad(x, total, opposite):
        g = 0.5 * LOGIT_SCALE * total - LOGIT_SCALE * opposite.astype(F32)
        return unit_back(x, g)

    image_out[...] = finish_grad(image, image_pull, text_unit)
    text_out[...] = finish_grad(text, text_pull, image_unit)
    lax.fori_loop(1, n, lse_drain, 0)
    drain(*i_set)
    drain(*t_set)


def body(captions, caption_layout, images, w_query, w_keyval, w_out, w_up, w_down, w_proj):
    captions = jnp.swapaxes(captions, 0, 1)
    ctx, caps, width = captions.shape
    n = lax.axis_size("dp")
    half = n // 2
    loads = CAP_CHUNKS + 4 + 2 * FF_CHUNKS
    any_spec = pl.BlockSpec(memory_space=pl.ANY)
    vmem = pl.BlockSpec(memory_space=pltpu.VMEM)
    smem = pl.BlockSpec(memory_space=pltpu.SMEM)
    out = jax.ShapeDtypeStruct(images.shape, F32)
    dma = pltpu.SemaphoreType.DMA
    return pl.pallas_call(
        functools.partial(kernel, n),
        out_shape=(out, out),
        in_specs=[any_spec, smem, vmem] + [any_spec] * 6,
        out_specs=(vmem, vmem),
        scratch_shapes=[
            pltpu.VMEM(captions.shape, BF16),
            pltpu.VMEM((caps // GROUP, ctx, GROUP, width), BF16),
            pltpu.VMEM((HEADS, caps, width), F32),
            pltpu.VMEM((HEADS, caps, width), F32),
            pltpu.VMEM(w_query.shape, BF16),
            pltpu.VMEM(w_keyval.shape, BF16),
            pltpu.VMEM(w_out.shape, BF16),
            pltpu.VMEM(w_up.shape, BF16),
            pltpu.VMEM(w_down.shape, BF16),
            pltpu.VMEM(w_proj.shape, BF16),
            pltpu.VMEM((n, caps, width), BF16),
            pltpu.VMEM((n, caps, width), BF16),
            pltpu.VMEM((n, 2, 128), F32),
            dma((loads,)),
            dma((n,)),
            dma((n,)),
        ]
        + [dma((half,)) for _ in range(8)],
        compiler_params=pltpu.CompilerParams(
            collective_id=0, has_side_effects=True, vmem_limit_bytes=64000000
        ),
    )(captions, caption_layout, images, w_query, w_keyval, w_out, w_up, w_down, w_proj)


def solution(mesh):
    return jax.shard_map(
        body,
        mesh=mesh,
        in_specs=(P("dp", None, None), P(), P("dp", None), P(), P(), P(), P(), P(), P()),
        out_specs=(P("dp", None), P("dp", None)),
        check_vma=False,
    )
```

```python
import functools

import jax
import jax.numpy as jnp
from jax import lax
from jax.experimental import pallas as pl
from jax.experimental.pallas import tpu as pltpu
from jax.sharding import PartitionSpec as P

HEADS = 12
LOGIT_SCALE = 100.0
EPS_NORM = 1e-05
EPS_UNIT = 1e-06
GROUP = 16
CAP_CHUNKS = 11
QUAD = 4
FF_CHUNKS = 4
MESH = pl.DeviceIdType.MESH
F32 = jnp.float32
BF16 = jnp.bfloat16


def dot(a, b):
    return jnp.dot(a, b, preferred_element_type=F32)


def dot_last(a, b):
    return lax.dot_general(a, b, (((1,), (1,)), ((), ())), preferred_element_type=F32)


def dot_first(a, b):
    return lax.dot_general(a, b, (((0,), (0,)), ((), ())), preferred_element_type=F32)


def layer_norm(x):
    center = x - jnp.mean(x, axis=-1, keepdims=True)
    spread = jnp.mean(center * center, axis=-1, keepdims=True)
    return center * lax.rsqrt(spread + EPS_NORM)


def unit_rows(x):
    return x * lax.rsqrt(jnp.sum(x * x, axis=-1, keepdims=True) + EPS_UNIT)


def unit_back(x, g):
    s = jnp.sum(x * x, axis=-1, keepdims=True) + EPS_UNIT
    r = lax.rsqrt(s)
    return g * r - x * (jnp.sum(x * g, axis=-1, keepdims=True) * (r / s))


def kernel(
    n,
    cap_hbm, layout, images, wq_hbm, wkv_hbm, wo_hbm, wup_hbm, wdown_hbm, wproj_hbm,
    image_out, text_out,
    cap, normed, qk, mix, wq, wkv, wo, wup, wdown, wproj,
    gi, gt, lse,
    load_sem, l_send, l_recv, i_send, i_recv, i_rsend, i_rrecv, t_send, t_recv, t_rsend, t_rrecv,
):
    me = lax.axis_index("dp")
    half = n // 2
    partner = me + 1 - 2 * lax.rem(me, 2)
    ctx, caps, width = cap.shape
    groups = caps // GROUP
    head_dim = width // HEADS
    ff = wup.shape[1]
    fc = ff // FF_CHUNKS

    loads = []

    def load(src, dst):
        copy = pltpu.make_async_copy(src, dst, load_sem.at[len(loads)])
        copy.start()
        loads.append(copy)
        return copy

    cap_steps = ctx // CAP_CHUNKS
    cap_loads = [
        load(cap_hbm.at[pl.ds(i * cap_steps, cap_steps)], cap.at[pl.ds(i * cap_steps, cap_steps)])
        for i in range(CAP_CHUNKS)
    ]
    wq_load = load(wq_hbm, wq)
    wkv_load = load(wkv_hbm, wkv)
    wo_load = load(wo_hbm, wo)
    ff_loads = []
    for f in range(FF_CHUNKS):
        cols = pl.ds(f * fc, fc)
        ff_loads.append(
            (load(wup_hbm.at[:, cols], wup.at[:, cols]), load(wdown_hbm.at[cols], wdown.at[cols]))
        )
    wproj_load = load(wproj_hbm, wproj)

    barrier = pltpu.get_barrier_semaphore()

    def greet(k, carry):
        pl.semaphore_signal(
            barrier, inc=1, device_id=(lax.rem(me + k, n),), device_id_type=MESH
        )
        return carry

    lax.fori_loop(1, n, greet, 0)

    def remote(buf, block, send, recv, target):
        return pltpu.make_async_remote_copy(
            src_ref=buf.at[block], dst_ref=buf.at[block], send_sem=send, recv_sem=recv,
            device_id=(target,), device_id_type=MESH,
        )

    depth = n // 8
    side = me + 2 - 4 * lax.rem(me // 2, 2)
    over = me + 4 - 8 * lax.rem(me // 4, 2)
    across = side + over - me
    upper = (0, caps // 2)
    lower = (caps // 2, caps // 2)

    def shift(base, k):
        return lax.rem(base + n - 8 * k, n)

    def move(buf, block, send, recv, index, target, part):
        ref = buf.at[block, pl.ds(*part)]
        return pltpu.make_async_remote_copy(
            src_ref=ref, dst_ref=ref, send_sem=send.at[index], recv_sem=recv.at[index],
            device_id=(target,), device_id_type=MESH,
        )

    def push(buf, send, recv, rsend, rrecv):
        def step(k, carry):
            remote(buf, me, send.at[k], recv.at[k], lax.rem(me + 8 * k, n)).start()
            return carry

        remote(buf, me, send.at[depth], recv.at[depth], side).start()
        remote(buf, me, send.at[2 * depth], recv.at[2 * depth], over).start()
        lax.fori_loop(1, depth, step, 0)
        remote(buf, me, rsend.at[0], rrecv.at[0], partner).start()

    def relay(buf, send, recv, rsend, rrecv):
        def first(k, carry):
            block = shift(me, k)
            remote(buf, block, send.at[k], recv.at[k], partner).wait_recv()
            remote(buf, block, send.at[depth + k], recv.at[depth + k], side).start()
            remote(buf, block, send.at[2 * depth + k], recv.at[2 * depth + k], over).start()
            remote(buf, block, rsend.at[k], rrecv.at[k], partner).start()
            return carry

        def second(k, carry):
            for kind, base, target, part in ((1, side, over, upper), (2, over, side, lower)):
                block = shift(base, k)
                place = kind * depth + k
                remote(buf, block, send.at[place], recv.at[place], partner).wait_recv()
                move(buf, block, send, recv, (kind + 2) * depth + k, target, part).start()
                remote(buf, block, rsend.at[place], rrecv.at[place], partner).start()
            return carry

        def third(k, carry):
            block = shift(across, k)
            move(buf, block, send, recv, 3 * depth + k, partner, upper).wait_recv()
            move(buf, block, send, recv, 4 * depth + k, partner, lower).wait_recv()
            place = 3 * depth + k
            remote(buf, block, rsend.at[place], rrecv.at[place], partner).start()
            return carry

        lax.fori_loop(1, depth, first, 0)
        lax.fori_loop(0, depth, second, 0)
        lax.fori_loop(0, depth, third, 0)

    def finish(buf, send, recv, rsend, rrecv):
        def step(k, carry):
            for kind, base in enumerate((me, side, over, across)):
                block = shift(base + partner - me, k)
                place = kind * depth + k
                remote(buf, block, rsend.at[place], rrecv.at[place], partner).wait_recv()
            return carry

        lax.fori_loop(0, depth, step, 0)

    def drain(buf, send, recv, rsend, rrecv):
        def step(k, carry):
            for kind, base in enumerate((me, side, over, across)):
                block = shift(base, k)
                place = kind * depth + k
                remote(buf, block, rsend.at[place], rrecv.at[place], partner).wait_send()
            for kind in (1, 2):
                place = kind * depth + k
                remote(buf, me, send.at[place], recv.at[place], partner).wait_send()
            move(buf, me, send, recv, 3 * depth + k, partner, upper).wait_send()
            move(buf, me, send, recv, 4 * depth + k, partner, lower).wait_send()
            return carry

        def near(k, carry):
            remote(buf, me, send.at[k], recv.at[k], partner).wait_send()
            return carry

        lax.fori_loop(1, depth, near, 0)
        lax.fori_loop(0, depth, step, 0)

    i_set = (gi, i_send, i_recv, i_rsend, i_rrecv)
    t_set = (gt, t_send, t_recv, t_rsend, t_rrecv)

    image = images[...].astype(F32)
    image_unit = unit_rows(image).astype(BF16)
    gi[me] = image_unit
    pl.semaphore_wait(barrier, n - 1)
    push(*i_set)

    row = lax.broadcasted_iota(jnp.int32, (caps, 128), 0)
    length_rows = jnp.zeros((caps, 128), jnp.int32)
    for c in range(caps):
        length_rows = jnp.where(row == c, layout[0, me * caps + c], length_rows)
    length_rows = jnp.concatenate([length_rows] * (width // 128), axis=1)

    last = jnp.zeros((caps, width), F32)
    for i in range(CAP_CHUNKS):
        cap_loads[i].wait()
        for t in range(i * cap_steps, (i + 1) * cap_steps):
            x = cap[t].astype(F32)
            last = jnp.where(length_rows == t + 1, x, last)
            y = layer_norm(x).astype(BF16)
            for g in range(groups):
                normed[g, t] = y[g * GROUP : (g + 1) * GROUP]
    last_normed = layer_norm(last).astype(BF16)
    wq_load.wait()
    query = dot(last_normed, wq[...]).astype(BF16).astype(F32) * (head_dim ** -0.5)
    wkv_load.wait()
    span = QUAD * head_dim
    lane = lax.broadcasted_iota(jnp.int32, (caps, span), 1)
    for b in range(HEADS // QUAD):
        piece = query[:, b * span : (b + 1) * span]
        stacked = jnp.concatenate(
            [
                jnp.where((lane >= j * head_dim) & (lane < (j + 1) * head_dim), piece, 0.0)
                for j in range(QUAD)
            ],
            axis=0,
        ).astype(BF16)
        part = dot_last(stacked, wkv[:, b * span : (b + 1) * span])
        qk[b * QUAD : (b + 1) * QUAD] = part.reshape(QUAD, caps, width)

    cols = HEADS * GROUP
    col_cap = lax.rem(lax.broadcasted_iota(jnp.int32, (1, cols), 1), GROUP)
    row_index = lax.broadcasted_iota(jnp.int32, (ctx * GROUP, cols), 0)
    same = lax.rem(row_index, GROUP) == col_cap

    for g in range(groups):
        rows = normed[g].reshape(ctx * GROUP, width)
        keys = qk[:, g * GROUP : (g + 1) * GROUP, :].reshape(cols, width).astype(BF16)
        scores = dot_last(rows, keys)
        lengths = jnp.zeros((1, cols), jnp.int32)
        for i in range(GROUP):
            lengths = jnp.where(col_cap == i, layout[0, me * caps + g * GROUP + i], lengths)
        inside = same & (row_index < lengths * GROUP)
        scores = jnp.where(inside, scores, -1e30)
        peak = jnp.max(scores, axis=0, keepdims=True)
        expo = jnp.where(inside, jnp.exp(scores - peak), 0.0)
        attn = (expo / jnp.sum(expo, axis=0, keepdims=True)).astype(BF16)
        mix[:, g * GROUP : (g + 1) * GROUP, :] = dot_first(attn, rows).reshape(HEADS, GROUP, width)

    pieces = []
    for b in range(HEADS // QUAD):
        left = mix[b * QUAD : (b + 1) * QUAD].reshape(QUAD * caps, width).astype(BF16)
        wide = dot(left, wkv[:, width + b * span : width + (b + 1) * span])
        piece = wide[:caps]
        for j in range(1, QUAD):
            piece = jnp.where(lane >= j * head_dim, wide[j * caps : (j + 1) * caps], piece)
        pieces.append(piece)
    mixed = jnp.concatenate(pieces, axis=1).astype(BF16)
    wo_load.wait()
    residual = (last + dot(mixed, wo[...])).astype(BF16).astype(F32)
    inner = layer_norm(residual).astype(BF16)

    relay(*i_set)

    final = residual
    for f in range(FF_CHUNKS):
        up_load, down_load = ff_loads[f]
        up_load.wait()
        up = dot(inner, wup[:, f * fc : (f + 1) * fc])
        hidden = (0.5 * up * (1.0 + lax.erf(up * (2.0 ** -0.5)))).astype(BF16)
        down_load.wait()
        final = final + dot(hidden, wdown[f * fc : (f + 1) * fc])
    pooled = layer_norm(final).astype(BF16)
    wproj_load.wait()
    text = dot(pooled, wproj[...]).astype(BF16).astype(F32)
    text_unit = unit_rows(text).astype(BF16)
    gt[me] = text_unit
    push(*t_set)
    finish(*i_set)

    pairs = gi.shape[0] * gi.shape[1]
    per_row = 128 // caps
    spot = lax.broadcasted_iota(jnp.int32, (caps, 128), 1) - lax.rem(me, per_row) * caps
    here = spot == row

    def score(mine, others):
        s = LOGIT_SCALE * dot_last(mine, others[...].reshape(pairs, width))
        peak = jnp.max(s, axis=1, keepdims=True)
        own = peak + jnp.log(jnp.sum(jnp.exp(s - peak), axis=1, keepdims=True))
        return s, own

    def pull(s, logsum, others):
        weights = jnp.exp(s - logsum).astype(BF16)
        return dot(weights, others[...].reshape(pairs, width))

    def as_lanes(own):
        return jnp.sum(jnp.where(here, own, 0.0), axis=0, keepdims=True)

    text_scores, col_own = score(text_unit, gi)
    text_pull = pull(text_scores, col_own, gi)
    relay(*t_set)
    finish(*t_set)
    image_scores, row_own = score(image_unit, gt)
    lse[me] = jnp.concatenate([as_lanes(row_own), as_lanes(col_own)], axis=0)

    def lse_copy(k, block, target):
        return pltpu.make_async_remote_copy(
            src_ref=lse.at[block], dst_ref=lse.at[block], send_sem=l_send.at[k],
            recv_sem=l_recv.at[k], device_id=(target,), device_id_type=MESH,
        )

    def lse_send(k, carry):
        lse_copy(k, me, lax.rem(me + k, n)).start()
        return carry

    def lse_wait(k, carry):
        lse_copy(k, lax.rem(me + n - k, n), partner).wait_recv()
        return carry

    def lse_drain(k, carry):
        lse_copy(k, me, partner).wait_send()
        return carry

    lax.fori_loop(1, n, lse_send, 0)
    image_pull = pull(image_scores, row_own, gt)
    lax.fori_loop(1, n, lse_wait, 0)
    rows_cols = [
        sum(lse[d] for d in range(start, start + per_row)) for start in range(0, n, per_row)
    ]
    every = jnp.concatenate(rows_cols, axis=1)
    image_pull = image_pull + pull(image_scores, every[1:2], gt)
    text_pull = text_pull + pull(text_scores, every[0:1], gi)

    def finish_grad(x, total, opposite):
        g = 0.5 * LOGIT_SCALE * total - LOGIT_SCALE * opposite.astype(F32)
        return unit_back(x, g)

    image_out[...] = finish_grad(image, image_pull, text_unit)
    text_out[...] = finish_grad(text, text_pull, image_unit)
    lax.fori_loop(1, n, lse_drain, 0)
    drain(*i_set)
    drain(*t_set)


def body(captions, caption_layout, images, w_query, w_keyval, w_out, w_up, w_down, w_proj):
    captions = jnp.swapaxes(captions, 0, 1)
    ctx, caps, width = captions.shape
    n = lax.axis_size("dp")
    half = n // 2
    loads = CAP_CHUNKS + 4 + 2 * FF_CHUNKS
    any_spec = pl.BlockSpec(memory_space=pl.ANY)
    vmem = pl.BlockSpec(memory_space=pltpu.VMEM)
    smem = pl.BlockSpec(memory_space=pltpu.SMEM)
    out = jax.ShapeDtypeStruct(images.shape, F32)
    dma = pltpu.SemaphoreType.DMA
    return pl.pallas_call(
        functools.partial(kernel, n),
        out_shape=(out, out),
        in_specs=[any_spec, smem, vmem] + [any_spec] * 6,
        out_specs=(vmem, vmem),
        scratch_shapes=[
            pltpu.VMEM(captions.shape, BF16),
            pltpu.VMEM((caps // GROUP, ctx, GROUP, width), BF16),
            pltpu.VMEM((HEADS, caps, width), F32),
            pltpu.VMEM((HEADS, caps, width), F32),
            pltpu.VMEM(w_query.shape, BF16),
            pltpu.VMEM(w_keyval.shape, BF16),
            pltpu.VMEM(w_out.shape, BF16),
            pltpu.VMEM(w_up.shape, BF16),
            pltpu.VMEM(w_down.shape, BF16),
            pltpu.VMEM(w_proj.shape, BF16),
            pltpu.VMEM((n, caps, width), BF16),
            pltpu.VMEM((n, caps, width), BF16),
            pltpu.VMEM((n, 2, 128), F32),
            dma((loads,)),
            dma((n,)),
            dma((n,)),
        ]
        + [dma((count,)) for count in (5 * n // 8, 5 * n // 8, half, half) * 2],
        compiler_params=pltpu.CompilerParams(
            collective_id=0, has_side_effects=True, vmem_limit_bytes=64000000
        ),
    )(captions, caption_layout, images, w_query, w_keyval, w_out, w_up, w_down, w_proj)


def solution(mesh):
    return jax.shard_map(
        body,
        mesh=mesh,
        in_specs=(P("dp", None, None), P(), P("dp", None), P(), P(), P(), P(), P(), P()),
        out_specs=(P("dp", None), P("dp", None)),
        check_vma=False,
    )
```
